32 devices in a mesh: fsdp: 8 (over z, core), tp: 4 (over y, x).
Axes of the slice: x: 2, y: 2, z: 4, core: 2. Of those that a mesh axis runs over, the one named last changes fastest.
Arguments:
- tokens: bfloat16 [80, 16384], P('tp', 'fsdp'), may hold values from -6 to 6
- gate_weight: bfloat16 [16384, 28672], P('fsdp', 'tp'), may hold values from -0.046875 to 0.046875
- up_weight: bfloat16 [16384, 28672], P('fsdp', 'tp'), may hold values from -0.046875 to 0.046875
- down_weight: bfloat16 [28672, 16384], P('tp', 'fsdp'), may hold values from -0.03125 to 0.03125
Outputs:
- layer_out: bfloat16 [80, 16384], P('tp', 'fsdp')
The draws below stay inside these ranges and needn't reach their ends.
All inputs are finite; a program needn't handle non-finite values.
Results may differ from the reference program's by a relative error of at most 0.019.
Values may be sent and summed in bfloat16 or wider, within the bound.
No kernel may reach another device: no remote copies, remote signals or barrier semaphores. Data moves between devices by JAX's collectives and lax.ppermute only.
A program may use at most 128 MiB of HBM per device.

```python
import jax
import jax.numpy as jnp

D = 16384
FF = 28672
TOKENS = 80


def levels(rng, dims, split, least, high):
    factor_of, own = 1.0, jax.random.fold_in(rng, 6)
    for dim, blocks in split:
        draws = jnp.exp(jax.random.uniform(jax.random.fold_in(own, dim), (blocks,), jnp.float32, least / len(split), high / len(split)))
        factor_of = factor_of * jnp.repeat(draws, dims[dim] // blocks).reshape([-1 if axis == dim else 1 for axis in range(len(dims))])
    return factor_of


def normal_values(stream_key, extent, deviation, limit, pieces=(), dtype=jnp.bfloat16):
    result = deviation * jax.random.normal(stream_key, extent, jnp.float32)
    if pieces:
        result = result * levels(stream_key, extent, pieces, -0.22, 0.18)
    return jnp.clip(result, -limit, limit).astype(dtype)


def setup_inputs(seed: int = 0) -> dict:
    key_of = jax.random.split(jax.random.key(seed), 5)
    return {
        "tokens": normal_values(key_of[0], (TOKENS, D), 1.0, 6.0, ((0, 4), (1, 8))),
        "gate_weight": normal_values(key_of[1], (D, FF), D ** -0.5, 0.046875, ((0, 8), (1, 4))),
        "up_weight": normal_values(key_of[2], (D, FF), D ** -0.5, 0.046875, ((0, 8), (1, 4))),
        "down_weight": normal_values(key_of[3], (FF, D), FF ** -0.5, 0.03125, ((0, 4), (1, 8))),
    }


def reference(tokens, gate_weight, up_weight, down_weight):
    gate_sum = jnp.dot(tokens, gate_weight, preferred_element_type=jnp.float32)
    up_sum = jnp.dot(tokens, up_weight, preferred_element_type=jnp.float32)
    hidden = (jax.nn.silu(gate_sum) * up_sum).astype(jnp.bfloat16)
    return jnp.dot(hidden, down_weight, preferred_element_type=jnp.float32).astype(jnp.bfloat16)
```

```python
import jax
import jax.numpy as jnp
from jax import lax
from jax.experimental import pallas as pl
from jax.experimental.pallas import tpu as pltpu
from jax.sharding import PartitionSpec as P

F32, BF16 = jnp.float32, jnp.bfloat16


def plain(tokens, gate_weight, up_weight, down_weight):
    segment = lax.all_gather(tokens, "tp", axis=0, tiled=True)
    gate_part = jnp.dot(segment, gate_weight, preferred_element_type=F32)
    up_part = jnp.dot(segment, up_weight, preferred_element_type=F32)
    partials = jnp.stack([gate_part, up_part])
    summed = lax.psum_scatter(partials, "fsdp", scatter_dimension=2, tiled=True)
    hidden = (jax.nn.silu(summed[0]) * summed[1]).astype(BF16)
    outputs = jnp.dot(
        lax.all_gather(hidden, "fsdp", axis=1, tiled=True),
        down_weight,
        preferred_element_type=F32,
    )
    return lax.psum_scatter(outputs.astype(BF16), "tp", scatter_dimension=0, tiled=True)


def tile_of(size, most):
    return next((t for t in range(most, 0, -128) if size % t == 0), size)


def gate_up(tokens, gate, up, pick, width, adds, dtypes, name):
    rows, depth = tokens.shape
    tk = tile_of(depth, 512)
    steps = depth // tk
    count = len(adds)
    given = [a for a in adds if a is not None]

    def body(tok, g, u, *rest):
        add_refs = list(rest[: len(given)])
        outs = rest[len(given) : len(given) + count]
        acc, wg, wu, sems = rest[len(given) + count :]
        blocks = pick()
        copies = []
        for b in range(count):
            at = pl.ds(pl.multiple_of(blocks[b] * width, 128), width)
            for k in range(steps):
                i = b * steps + k
                span = pl.ds(k * tk, tk)
                pair = (
                    pltpu.make_async_copy(g.at[span, at], wg.at[i], sems.at[0, i]),
                    pltpu.make_async_copy(u.at[span, at], wu.at[i], sems.at[1, i]),
                )
                for copy in pair:
                    copy.start()
                copies.append(pair)
        for b in range(count):
            for k in range(steps):
                i = b * steps + k
                t = tok[:, k * tk : (k + 1) * tk]
                for half, w in ((0, wg), (1, wu)):
                    copies[i][half].wait()
                    part = jnp.dot(t, w[i], preferred_element_type=F32)
                    acc[half] = part if k == 0 else acc[half] + part
            value = acc[...]
            if adds[b] is not None:
                value = value + add_refs.pop(0)[...].astype(F32)
            outs[b][...] = value.astype(dtypes[b])

    vmem = pl.BlockSpec(memory_space=pltpu.VMEM)
    hbm = pl.BlockSpec(memory_space=pl.ANY)
    return pl.pallas_call(
        body,
        in_specs=[vmem, hbm, hbm] + [vmem] * len(given),
        out_specs=[vmem] * count,
        scratch_shapes=[
            pltpu.VMEM((2, rows, width), F32),
            pltpu.VMEM((count * steps, tk, width), BF16),
            pltpu.VMEM((count * steps, tk, width), BF16),
            pltpu.SemaphoreType.DMA((2, count * steps)),
        ],
        out_shape=[jax.ShapeDtypeStruct((2, rows, width), d) for d in dtypes],
        cost_estimate=pl.CostEstimate(
            flops=4 * rows * depth * width * count,
            bytes_accessed=4 * depth * width * count,
            transcendentals=0,
        ),
        name=name,
    )(tokens, gate, up, *given)


def down(hiddens, weight, pick, so_far, name, dtype=F32):
    rows, width = hiddens[0].shape
    cols = weight.shape[1]
    tn = tile_of(cols, 512)
    steps = cols // tn
    count = len(hiddens)

    def body(w, *rest):
        hs = rest[:count]
        before = rest[count] if so_far is not None else None
        out, tiles, sems = rest[-3:]
        blocks = pick()
        copies = []
        for b in range(count):
            at = pl.ds(pl.multiple_of(blocks[b] * width, 128), width)
            for j in range(steps):
                i = b * steps + j
                copy = pltpu.make_async_copy(
                    w.at[at, pl.ds(j * tn, tn)], tiles.at[i], sems.at[i]
                )
                copy.start()
                copies.append(copy)
        for b in range(count):
            for j in range(steps):
                i = b * steps + j
                span = slice(j * tn, (j + 1) * tn)
                copies[i].wait()
                part = jnp.dot(hs[b][...], tiles[i], preferred_element_type=F32)
                if b > 0:
                    part = part + out[:, span]
                elif before is not None:
                    part = part + before[:, span]
                out[:, span] = part.astype(dtype)

    vmem = pl.BlockSpec(memory_space=pltpu.VMEM)
    extra = [] if so_far is None else [so_far]
    return pl.pallas_call(
        body,
        in_specs=[pl.BlockSpec(memory_space=pl.ANY)] + [vmem] * (count + len(extra)),
        out_specs=vmem,
        scratch_shapes=[
            pltpu.VMEM((count * steps, width, tn), BF16),
            pltpu.SemaphoreType.DMA((count * steps,)),
        ],
        out_shape=jax.ShapeDtypeStruct((rows, cols), dtype),
        cost_estimate=pl.CostEstimate(
            flops=2 * rows * width * cols * count,
            bytes_accessed=2 * width * cols * count,
            transcendentals=0,
        ),
        name=name,
    )(weight, *hiddens, *extra)


def split(n, tp):
    pairs = n // 2
    swap = [(j, j ^ 1) for j in range(n)]

    def own(o):
        me = lax.axis_index("fsdp")
        return 2 * ((me // 2 + o) % pairs) + me % 2

    def other(o):
        me = lax.axis_index("fsdp")
        return 2 * ((me // 2 + o) % pairs) + 1 - me % 2

    def shift(x, o):
        perm = [(j, 2 * ((j // 2 + o) % pairs) + j % 2) for j in range(n)]
        return lax.ppermute(x, "fsdp", perm)

    def trade(x):
        return lax.ppermute(x, "fsdp", swap)

    def peer(x, k):
        return lax.ppermute(x, "tp", [(j, j ^ k) for j in range(tp)])

    return pairs, own, other, shift, trade, peer


def per_device(n, tp, tokens, gate_weight, up_weight, down_weight):
    pairs, own, other, shift, trade, peer = split(n, tp)
    width = gate_weight.shape[1] // n
    mine = tokens.shape[0]
    segment = jnp.concatenate([tokens] + [peer(tokens, k) for k in range(1, tp)])

    order = sorted(range(1, pairs), key=lambda o: (-min(o, pairs - o), o)) + [0]
    calls = [[("to", order[0]), ("to", order[1])]]
    for i in range(1, pairs - 1):
        calls.append([("at", order[i - 1]), ("to", order[i + 1])])
    if pairs > 2:
        calls[-1] = [("at", order[-3]), ("at", order[-2])]
        calls.append([("to", 0), ("at", 0)])
    else:
        calls.append([("at", order[0]), ("at", 0)])
    arrived = {}
    received = []
    for i, call in enumerate(calls):
        parts = gate_up(
            segment,
            gate_weight,
            up_weight,
            lambda: [own(o) if kind == "at" else other(o) for kind, o in call],
            width,
            [arrived[o] if kind == "at" and o else None for kind, o in call],
            [F32 if kind == "at" and not o else BF16 for kind, o in call],
            f"gu{i}",
        )
        segment, *parts = lax.optimization_barrier([segment, *parts])
        for (kind, o), part in zip(call, parts):
            if kind == "to":
                arrived[o] = trade(part)
            elif o:
                received.append(shift(part, o))
            else:
                total = part
    for part in received + [arrived[0]]:
        total = total + part.astype(F32)
    hidden = (jax.nn.silu(total[0]) * total[1]).astype(BF16)

    rest = order[:-1][::-1]
    beside = trade(hidden)
    straight = {o: shift(hidden, -o) for o in rest}
    near, far = rest[:-1], rest[-1]
    outputs = down([hidden], down_weight, lambda: [own(0)], None, "down0")
    *held, outputs = lax.optimization_barrier([straight[o] for o in near] + [outputs])
    crossed = [trade(x) for x in held]
    outputs = down(
        [beside] + held,
        down_weight,
        lambda: [other(0)] + [own(o) for o in near],
        outputs,
        "down1",
    )
    distant, outputs = lax.optimization_barrier((straight[far], outputs))
    final = trade(distant)
    outputs = down(
        crossed + [distant],
        down_weight,
        lambda: [other(o) for o in near] + [own(far)],
        outputs,
        "down2",
    )
    outputs = down([final], down_weight, lambda: [other(far)], outputs, "down3", BF16)
    rows = [outputs[k * mine : (k + 1) * mine] for k in range(tp)]
    result = rows[0].astype(F32)
    for k in range(1, tp):
        result = result + peer(rows[k], k).astype(F32)
    return result.astype(BF16)


def solution(mesh):
    n, tp = mesh.shape["fsdp"], mesh.shape["tp"]

    def body(tokens, gate_weight, up_weight, down_weight):
        width = gate_weight.shape[1] // n
        fits = n % 2 == 0 and n >= 4 and tp & (tp - 1) == 0 and width % 128 == 0
        fits = fits and tokens.shape[1] % 128 == 0 and (tp * tokens.shape[0]) % 16 == 0
        if not fits:
            return plain(tokens, gate_weight, up_weight, down_weight)
        return per_device(n, tp, tokens, gate_weight, up_weight, down_weight)

    placed = (P("tp", "fsdp"), P("fsdp", "tp"), P("fsdp", "tp"), P("tp", "fsdp"))
    return jax.shard_map(
        body, mesh=mesh, in_specs=placed, out_specs=P("tp", "fsdp"), check_vma=False
    )
```
